32 devices in a mesh: seq: 8 (over y, x, core), tensor: 4 (over z).
Axes of the slice: x: 2, y: 2, z: 4, core: 2. Of those that a mesh axis runs over, the one named last changes fastest.
Arguments:
- tokens: bfloat16 [5760, 1536], P('seq'), may hold values from -6 to 6
- norm_gain: float32 [1536], replicated, may hold values from 0.1 to 1.9
- w_qkv: bfloat16 [1536, 3, 1536], P(None, None, 'tensor'), may hold values from -8 to 8
- w_out: bfloat16 [1536, 1536], P('tensor'), may hold values from -0.15625 to 0.15625
- post_gain: float32 [1536], replicated, may hold values from 0.1 to 1.9
- w_up: bfloat16 [1536, 6144], P(None, 'tensor'), may hold values from -0.15625 to 0.15625
- w_down: bfloat16 [6144, 1536], P('tensor'), may hold values from -0.078125 to 0.078125
Outputs:
- layer_out: bfloat16 [5760, 1536], P('seq')
The draws below stay inside these ranges and needn't reach their ends.
All inputs are finite; a program needn't handle non-finite values.
Results may differ from the reference program's by a relative error of at most 0.015.
Values may be sent and summed in bfloat16 or wider, within the bound.
A program may use at most 128 MiB of HBM per device.

```python
import math
import jax
import jax.numpy as jnp
from jax import lax

D = 1536
HEADS = 32
HD = 48
FF = 6144
TOK_DEV = 720
TOKENS = 5760
N_TENSOR = 4


def draw_w_qkv(key, part):
    base = jax.random.normal(key, (D, 3, HEADS * HD), jnp.float32) * D ** (-0.5)
    levels = jax.random.uniform(jax.random.fold_in(key, 3), (HEADS,), jnp.float32, math.log(1.5), math.log(3.5))
    sharpness = jnp.repeat(jnp.exp(levels), HD)
    query = base[:, 0, :] * sharpness[None, :]
    stacked = jnp.stack([query, base[:, 1, :], base[:, 2, :]], axis=1)
    return jnp.clip(stacked, -8.0, 8.0).astype(jnp.bfloat16)


def level_of(stream_key, shape, cuts, least, top_value):
    def one(dim, parts):
        steps = jax.random.uniform(jax.random.fold_in(jax.random.fold_in(stream_key, 6), dim), (parts,), jnp.float32, least / len(cuts), top_value / len(cuts))
        return jnp.repeat(jnp.exp(steps), shape[dim] // parts).reshape((-1,) + (1,) * (len(shape) - dim - 1))

    level = one(*cuts[0])
    for cut in cuts[1:]:
        level = level * one(*cut)
    return level


def scatter_about(rng, extent, scale, bound, split=(), dtype=jnp.bfloat16):
    loudness = level_of(rng, extent, split, -0.22, 0.18) if split else 1.0
    array = jax.random.normal(rng, extent, jnp.float32) * scale * loudness
    return jnp.minimum(jnp.maximum(array, -bound), bound).astype(dtype)


def setup_inputs(seed: int = 0) -> dict:
    key_list = jax.random.split(jax.random.key(seed), 8)
    return {
        "tokens": scatter_about(key_list[0], (TOKENS, D), 1.0, 6.0, ((0, 8),)),
        "norm_gain": jnp.clip(1.0 + 0.18 * jax.random.normal(key_list[1], (D,), jnp.float32), 0.1, 1.9),
        "w_qkv": draw_w_qkv(jax.random.fold_in(key_list[7], 71), 0),
        "w_out": scatter_about(key_list[3], (HEADS * HD, D), (HEADS * HD) ** -0.5, 0.15625, ((0, 4),)),
        "post_gain": jnp.clip(1.0 + 0.18 * jax.random.normal(key_list[4], (D,), jnp.float32), 0.1, 1.9),
        "w_up": scatter_about(key_list[5], (D, FF), D ** -0.5, 0.15625, ((1, 4),)),
        "w_down": scatter_about(key_list[6], (FF, D), FF ** -0.5, 0.078125, ((0, 4),)),
    }


def layer_norm(values, gain):
    mean = lax.optimization_barrier(jnp.mean(values, axis=-1, keepdims=True))
    centred = values - mean
    var = lax.optimization_barrier(jnp.mean(centred * centred, axis=-1, keepdims=True))
    return centred * lax.rsqrt(var + 1e-05) * gain

def one_head(operands):
    query, key, value = operands
    scale = 1.0 / HD ** 0.5

    def block(query_block):
        scores = jnp.dot(query_block, key.T, preferred_element_type=jnp.float32) * scale
        peak = lax.optimization_barrier(jnp.max(scores, axis=-1, keepdims=True))
        weights = jnp.exp(scores - peak)
        total = lax.optimization_barrier(jnp.sum(weights, axis=-1, keepdims=True))
        return jnp.dot(weights.astype(jnp.bfloat16), value, preferred_element_type=jnp.float32) / total
    blocks = query.reshape(TOKENS // TOK_DEV, TOK_DEV, HD)
    return lax.map(block, blocks).reshape(TOKENS, HD)

def grouped_sum(left, right):
    width = left.shape[1] // N_TENSOR
    result = jnp.zeros((left.shape[0], right.shape[1]), jnp.float32)
    for group in range(N_TENSOR):
        term = jnp.dot(left[:, group * width:(group + 1) * width], right[group * width:(group + 1) * width], preferred_element_type=jnp.float32)
        term = lax.optimization_barrier(term.astype(jnp.bfloat16))
        result = result + term.astype(jnp.float32)
    return result

def reference(tokens, norm_gain, w_qkv, w_out, post_gain, w_up, w_down):
    base = tokens.astype(jnp.float32)
    normed = layer_norm(base, norm_gain).astype(jnp.bfloat16)
    qkv = jnp.dot(normed, w_qkv.reshape(D, 3 * HEADS * HD), preferred_element_type=jnp.float32).astype(jnp.bfloat16)
    qkv = qkv.reshape(TOKENS, 3, HEADS, HD)
    query = jnp.transpose(qkv[:, 0], (1, 0, 2))
    key = jnp.transpose(qkv[:, 1], (1, 0, 2))
    value = jnp.transpose(qkv[:, 2], (1, 0, 2))
    heads = lax.map(one_head, (query, key, value))
    attended = jnp.transpose(heads, (1, 0, 2)).reshape(TOKENS, HEADS * HD).astype(jnp.bfloat16)
    mixed = base + grouped_sum(attended, w_out)
    post = layer_norm(mixed, post_gain).astype(jnp.bfloat16)
    hidden = jax.nn.gelu(jnp.dot(post, w_up, preferred_element_type=jnp.float32), approximate=True).astype(jnp.bfloat16)
    return (mixed + grouped_sum(hidden, w_down)).astype(jnp.bfloat16)
```

```python
import functools

import jax
import jax.numpy as jnp
from jax import lax
from jax.experimental import pallas as pl
from jax.experimental.pallas import tpu as pltpu
from jax.sharding import PartitionSpec as P

HD = 48
ONES = 16
LOG2E = 1.4426950408889634
MESH = pl.DeviceIdType.MESH
CONTRACT_FIRST = (((0,), (0,)), ((), ()))


def layer_norm(values, gain):
    mean = jnp.mean(values, axis=-1, keepdims=True)
    centred = values - mean
    var = jnp.mean(centred * centred, axis=-1, keepdims=True)
    return centred * lax.rsqrt(var + 1e-05) * gain


def flip(chip, mask, chips):
    result, bit = 0, 1
    while bit < chips:
        mine, other = (chip // bit) % 2, (mask // bit) % 2
        result = result + bit * (mine + other - 2 * mine * other)
        bit *= 2
    return result


def attend_kernel(n, heads, group, q_ref, kv_ref, o_ref, held, accum, peak, own_sem, send_sem, pass_sem, recv_sem):
    seq, lane = lax.axis_index("seq"), lax.axis_index("tensor")
    chips = n // 2
    chip, core = seq // 2, seq % 2
    sibling = chip * 2 + 1 - core

    def order(step, which):
        if chips < 4:
            return step + 1
        return step + 1 + which * (jnp.where(step == 0, 1, 0) - jnp.where(step == 1, 1, 0))

    def send(source, slot, target, sem):
        return pltpu.make_async_remote_copy(
            src_ref=source,
            dst_ref=held.at[slot],
            send_sem=sem,
            recv_sem=recv_sem.at[slot],
            device_id=(target, lane),
            device_id_type=MESH,
        )

    barrier = pltpu.get_barrier_semaphore()
    pl.semaphore_signal(barrier, inc=1, device_id=(sibling, lane), device_id_type=MESH)
    for step in range(1, chips):
        pl.semaphore_signal(
            barrier, inc=1, device_id=(flip(chip, step, chips) * 2 + core, lane), device_id_type=MESH
        )
    pl.semaphore_wait(barrier, chips)

    for step in range(chips - 1):
        target = flip(chip, order(step, core), chips) * 2 + core
        send(kv_ref, seq, target, send_sem.at[step]).start()
    send(kv_ref, seq, sibling, pass_sem.at[chips - 1]).start()
    own = pltpu.make_async_copy(kv_ref, held.at[seq], own_sem)
    own.start()
    accum[...] = jnp.zeros_like(accum)
    peak[...] = jnp.full_like(peak, -1e30)
    own.wait()

    def attend(slot):
        @pl.loop(0, heads // group)
        def _(index):
            members = [index * group + offset for offset in range(group)]
            scores = [
                lax.dot_general(held[slot, h], q_ref[h], CONTRACT_FIRST, preferred_element_type=jnp.float32)
                for h in members
            ]
            for h, score in zip(members, scores):
                value = held[slot, heads + h]
                value = jnp.concatenate([value, jnp.ones((ONES, value.shape[1]), value.dtype)], axis=0)
                old = peak[h]
                new = jnp.maximum(old, jnp.max(score, axis=0, keepdims=True))
                weights = jnp.exp2(score - new).astype(jnp.bfloat16)
                term = jnp.dot(value, weights, preferred_element_type=jnp.float32)
                accum[h] = accum[h] * jnp.exp2(old - new) + term
                peak[h] = new

    @pl.loop(0, n)
    def _(index):
        step, second = index // 2, index % 2
        which = core + second - 2 * core * second
        mask = jnp.where(step == 0, 0, order(step - 1, which))
        slot = flip(chip, mask, chips) * 2 + which

        @pl.when(index > 0)
        def _():
            send(held.at[slot], slot, sibling, pass_sem.at[0]).wait_recv()

        @pl.when(jnp.logical_and(index > 0, second == 0))
        def _():
            send(held.at[slot], slot, sibling, pass_sem.at[step - 1]).start()

        attend(slot)

    for h in range(heads):
        o_ref[h] = (accum[h, :HD] / accum[h, HD : HD + 1]).astype(o_ref.dtype)

    for step in range(chips - 1):
        send(kv_ref, seq, sibling, send_sem.at[step]).wait_send()
    for step in range(chips):
        send(kv_ref, seq, sibling, pass_sem.at[step]).wait_send()


def attention(n, heads, query, pairs):
    rows = query.shape[2]
    group = next(size for size in (4, 2, 1) if heads % size == 0)
    vmem = pl.BlockSpec(memory_space=pltpu.VMEM)
    return pl.pallas_call(
        functools.partial(attend_kernel, n, heads, group),
        out_shape=jax.ShapeDtypeStruct((heads, HD, rows), jnp.bfloat16),
        in_specs=[vmem, vmem],
        out_specs=vmem,
        scratch_shapes=[
            pltpu.VMEM((n, 2 * heads, HD, rows), jnp.bfloat16),
            pltpu.VMEM((heads, HD + ONES, rows), jnp.float32),
            pltpu.VMEM((heads, 1, rows), jnp.float32),
            pltpu.SemaphoreType.DMA,
            pltpu.SemaphoreType.DMA((n // 2,)),
            pltpu.SemaphoreType.DMA((n // 2,)),
            pltpu.SemaphoreType.DMA((n,)),
        ],
        compiler_params=pltpu.CompilerParams(
            collective_id=0, has_side_effects=True, vmem_limit_bytes=56 * 2**20
        ),
    )(query, pairs)


def per_device(n, tokens, norm_gain, w_qkv, w_out, post_gain, w_up, w_down):
    rows = tokens.shape[0]
    span = w_qkv.shape[2]
    heads = span // HD
    base = tokens.astype(jnp.float32)
    normed = layer_norm(base, norm_gain).astype(jnp.bfloat16)
    weights = w_qkv.reshape(w_qkv.shape[0], -1)
    qkv = lax.dot_general(weights, normed, (((0,), (1,)), ((), ())), preferred_element_type=jnp.float32)
    query = (qkv[:span] * (LOG2E / HD**0.5)).astype(jnp.bfloat16).reshape(heads, HD, rows)
    pairs = qkv[span:].astype(jnp.bfloat16).reshape(2 * heads, HD, rows)
    attended = attention(n, heads, query, pairs).reshape(span, rows)
    attn_term = lax.dot_general(attended, w_out, CONTRACT_FIRST, preferred_element_type=jnp.float32)
    mixed = base + lax.psum(attn_term.astype(jnp.bfloat16), "tensor").astype(jnp.float32)
    post = layer_norm(mixed, post_gain).astype(jnp.bfloat16)
    hidden = jax.nn.gelu(
        jnp.dot(post, w_up, preferred_element_type=jnp.float32), approximate=True
    ).astype(jnp.bfloat16)
    mlp_term = jnp.dot(hidden, w_down, preferred_element_type=jnp.float32)
    return (mixed + lax.psum(mlp_term.astype(jnp.bfloat16), "tensor").astype(jnp.float32)).astype(
        jnp.bfloat16
    )


def solution(mesh):
    placed = (
        P("seq", None),
        P(),
        P(None, None, "tensor"),
        P("tensor", None),
        P(),
        P(None, "tensor"),
        P("tensor", None),
    )
    return jax.shard_map(
        functools.partial(per_device, mesh.shape["seq"]),
        mesh=mesh,
        in_specs=placed,
        out_specs=P("seq", None),
        check_vma=False,
    )
```

```python
import functools

import jax
import jax.numpy as jnp
from jax import lax
from jax.experimental import pallas as pl
from jax.experimental.pallas import tpu as pltpu
from jax.sharding import PartitionSpec as P


HD = 48
ONES = 16
LOG2E = 1.4426950408889634
MESH = pl.DeviceIdType.MESH
CONTRACT_FIRST = (((0,), (0,)), ((), ()))


def layer_norm(values, gain):
    mean = jnp.mean(values, axis=-1, keepdims=True)
    centred = values - mean
    var = jnp.mean(centred * centred, axis=-1, keepdims=True)
    return centred * lax.rsqrt(var + 1e-05) * gain


def flip(chip, mask, chips):
    result, bit = 0, 1
    while bit < chips:
        mine, other = (chip // bit) % 2, (mask // bit) % 2
        result = result + bit * (mine + other - 2 * mine * other)
        bit *= 2
    return result


def attend_kernel(n, heads, group, q_ref, kv_ref, o_ref, held, accum, peak, own_sem, send_sem, pass_sem, recv_sem):
    seq, lane = lax.axis_index("seq"), lax.axis_index("tensor")
    chips = n // 2
    chip, core = seq // 2, seq % 2
    sibling = chip * 2 + 1 - core

    def order(step, which):
        if chips < 4:
            return step + 1
        return step + 1 + which * (jnp.where(step == 0, 1, 0) - jnp.where(step == 1, 1, 0))

    def send(source, slot, target, sem):
        return pltpu.make_async_remote_copy(
            src_ref=source,
            dst_ref=held.at[slot],
            send_sem=sem,
            recv_sem=recv_sem.at[slot],
            device_id=(target, lane),
            device_id_type=MESH,
        )

    barrier = pltpu.get_barrier_semaphore()
    pl.semaphore_signal(barrier, inc=1, device_id=(sibling, lane), device_id_type=MESH)
    for step in range(1, chips):
        pl.semaphore_signal(
            barrier, inc=1, device_id=(flip(chip, step, chips) * 2 + core, lane), device_id_type=MESH
        )
    pl.semaphore_wait(barrier, chips)

    for step in range(chips - 1):
        target = flip(chip, order(step, core), chips) * 2 + core
        send(kv_ref, seq, target, send_sem.at[step]).start()
    send(kv_ref, seq, sibling, pass_sem.at[chips - 1]).start()
    own = pltpu.make_async_copy(kv_ref, held.at[seq], own_sem)
    own.start()
    accum[...] = jnp.zeros_like(accum)
    peak[...] = jnp.full_like(peak, -1e30)
    own.wait()

    def attend(slot):
        @pl.loop(0, heads // group)
        def _(index):
            members = [index * group + offset for offset in range(group)]
            scores = [
                lax.dot_general(held[slot, h], q_ref[h], CONTRACT_FIRST, preferred_element_type=jnp.float32)
                for h in members
            ]
            for h, score in zip(members, scores):
                value = held[slot, heads + h]
                value = jnp.concatenate([value, jnp.ones((ONES, value.shape[1]), value.dtype)], axis=0)
                old = peak[h]
                new = jnp.maximum(old, jnp.max(score, axis=0, keepdims=True))
                weights = jnp.exp2(score - new).astype(jnp.bfloat16)
                term = jnp.dot(value, weights, preferred_element_type=jnp.float32)
                accum[h] = accum[h] * jnp.exp2(old - new) + term
                peak[h] = new

    @pl.loop(0, n)
    def _(index):
        step, second = index // 2, index % 2
        which = core + second - 2 * core * second
        mask = jnp.where(step == 0, 0, order(step - 1, which))
        slot = flip(chip, mask, chips) * 2 + which

        @pl.when(index > 0)
        def _():
            send(held.at[slot], slot, sibling, pass_sem.at[0]).wait_recv()

        @pl.when(jnp.logical_and(index > 0, second == 0))
        def _():
            send(held.at[slot], slot, sibling, pass_sem.at[step - 1]).start()

        attend(slot)

    for h in range(heads):
        o_ref[h] = (accum[h, :HD] / accum[h, HD : HD + 1]).astype(o_ref.dtype)

    for step in range(chips - 1):
        send(kv_ref, seq, sibling, send_sem.at[step]).wait_send()
    for step in range(chips):
        send(kv_ref, seq, sibling, pass_sem.at[step]).wait_send()


def attention(n, heads, query, pairs):
    rows = query.shape[2]
    group = next(size for size in (4, 2, 1) if heads % size == 0)
    vmem = pl.BlockSpec(memory_space=pltpu.VMEM)
    return pl.pallas_call(
        functools.partial(attend_kernel, n, heads, group),
        out_shape=jax.ShapeDtypeStruct((heads, HD, rows), jnp.bfloat16),
        in_specs=[vmem, vmem],
        out_specs=vmem,
        scratch_shapes=[
            pltpu.VMEM((n, 2 * heads, HD, rows), jnp.bfloat16),
            pltpu.VMEM((heads, HD + ONES, rows), jnp.float32),
            pltpu.VMEM((heads, 1, rows), jnp.float32),
            pltpu.SemaphoreType.DMA,
            pltpu.SemaphoreType.DMA((n // 2,)),
            pltpu.SemaphoreType.DMA((n // 2,)),
            pltpu.SemaphoreType.DMA((n,)),
        ],
        compiler_params=pltpu.CompilerParams(
            collective_id=0, has_side_effects=True, vmem_limit_bytes=56 * 2**20
        ),
        cost_estimate=pl.CostEstimate(
            flops=4 * n * heads * rows * rows * HD,
            bytes_accessed=6 * heads * HD * rows,
            transcendentals=n * heads * rows * rows,
        ),
    )(query, pairs)


def per_device(n, tokens, norm_gain, w_qkv, w_out, post_gain, w_up, w_down):
    rows = tokens.shape[0]
    span = w_qkv.shape[2]
    heads = span // HD
    base = tokens.astype(jnp.float32)
    normed = layer_norm(base, norm_gain).astype(jnp.bfloat16)
    weights = w_qkv.reshape(w_qkv.shape[0], -1)
    qkv = lax.dot_general(weights, normed, (((0,), (1,)), ((), ())), preferred_element_type=jnp.float32)
    query = (qkv[:span] * (LOG2E / HD**0.5)).astype(jnp.bfloat16).reshape(heads, HD, rows)
    pairs = qkv[span:].astype(jnp.bfloat16).reshape(2 * heads, HD, rows)
    w_full = lax.all_gather(w_out, "tensor", axis=0, tiled=True)
    attended = attention(n, heads, query, pairs)
    attended = attended.reshape(span, rows)
    attended = lax.all_gather(attended, "tensor", axis=0, tiled=True)
    mixed = base + lax.dot_general(attended, w_full, CONTRACT_FIRST, preferred_element_type=jnp.float32)
    post = layer_norm(mixed, post_gain).astype(jnp.bfloat16)
    hidden = jax.nn.gelu(
        jnp.dot(post, w_up, preferred_element_type=jnp.float32), approximate=True
    ).astype(jnp.bfloat16)
    mlp_term = jnp.dot(hidden, w_down, preferred_element_type=jnp.float32)
    return (mixed + lax.psum(mlp_term.astype(jnp.bfloat16), "tensor").astype(jnp.float32)).astype(
        jnp.bfloat16
    )


def solution(mesh):
    placed = (
        P("seq", None),
        P(),
        P(None, None, "tensor"),
        P("tensor", None),
        P(),
        P(None, "tensor"),
        P("tensor", None),
    )
    return jax.shard_map(
        functools.partial(per_device, mesh.shape["seq"]),
        mesh=mesh,
        in_specs=placed,
        out_specs=P("seq", None),
        check_vma=False,
    )
```
